256 devices in a mesh: dp: 2 (over core), seq: 32 (over z, x), tensor: 4 (over y).
Axes of the slice: x: 4, y: 4, z: 8, core: 2. Of those that a mesh axis runs over, the one named last changes fastest.
Arguments:
- tokens: bfloat16 [2048, 4, 5120], P('seq', 'dp'), parts along dimension 1, may hold values from -6 to 6
- w_query: bfloat16 [5120, 5120], P(None, 'tensor'), may hold values from -0.5 to 0.5, as said below
- w_key: bfloat16 [5120, 5120], P(None, 'tensor'), may hold values from -0.5 to 0.5, as said below
- w_value: bfloat16 [5120, 5120], P(None, 'tensor'), may hold values from -0.078125 to 0.078125
- w_out: bfloat16 [5120, 5120], P('tensor'), may hold values from -0.125 to 0.125
- gain_query: float32 [5120], P('tensor'), may hold values from 0.5 to 4
- gain_key: float32 [5120], P('tensor'), may hold values from 0.5 to 4
Outputs:
- attended: bfloat16 [2048, 4, 5120], P(('seq', 'tensor'), 'dp'), parts along dimension 1
The draws below stay inside these ranges and needn't reach their ends.
There are 2 independent parts, one for each index of `dp`. The reference program is written for one: setup_inputs(seed, part) draws one part's arguments, and reference() takes and returns one part's arrays. A program takes and returns all parts, laid end to end along the dimension named above; an argument that names none is the same for every part. Nothing has to cross between parts.
Inputs may be any that keep to these rules, and one draw needn't show every extreme that they name: `w_query`: entries of order 5120 ** -0.5 with unequal column scales. `w_key`: entries of order 5120 ** -0.5 with unequal column scales.
All inputs are finite; a program needn't handle non-finite values.
Results may differ from the reference program's by a relative error of at most 0.013.
The reference program's roundings to bfloat16 on the way count: a program that leaves them out, or rounds other values in their place, can miss the bound.
Values may be sent and summed in bfloat16 or wider, within the bound.
No kernel may reach another device: no remote copies, remote signals or barrier semaphores. Data moves between devices by JAX's collectives and lax.ppermute only.
A program may use at most 256 MiB of HBM per device.

```python
import jax
import jax.numpy as jnp
from jax import lax

D = 5120
HEADS = 40
HEAD_DIM = 128
SEQS = 2
TOK_DEV = 64
SEQ = 2048


def ramped_weight(key, salt):
    width = HEADS * HEAD_DIM
    first, second = jax.random.split(jax.random.fold_in(key, salt))
    base = jax.random.truncated_normal(first, -4.0, 4.0, (D, width), jnp.float32)
    heads = (jnp.arange(width) // HEAD_DIM).astype(jnp.float32)
    ramp = jnp.exp(jnp.log(0.6) + jnp.log(3.0) * heads / max(HEADS - 1, 1))
    upper = 3.3
    column = jnp.exp(jax.random.uniform(second, (width,), jnp.float32) * jnp.log(upper))
    scaled = base * (ramp * column)[None, :] / jnp.sqrt(jnp.float32(D))
    return jnp.clip(scaled, -0.5, 0.5).astype(jnp.bfloat16)


def drawn_gain(key, salt):
    width = HEADS * HEAD_DIM
    lower, upper = (0.5, 2.0)
    sample = jax.random.uniform(jax.random.fold_in(key, salt), (width,), jnp.float32, jnp.log(lower), jnp.log(upper))
    return jnp.exp(sample).astype(jnp.float32)


def draw_w_query(key, part):
    return ramped_weight(key, 11)


def draw_w_key(key, part):
    return ramped_weight(key, 23)


def draw_gain_query(key, part):
    return drawn_gain(key, 37)


def draw_gain_key(key, part):
    return drawn_gain(key, 41)


def with_spikes(entries, rng, source, target, parts, factor):
    def block_of(axis_at):
        return (jnp.arange(entries.shape[axis_at]) // (entries.shape[axis_at] // parts)).reshape((-1,) + (1,) * (entries.ndim - 1 - axis_at))

    one_side = jax.random.permutation(rng, parts)[block_of(target)]
    other_side = (block_of(target) + parts // 2) % parts
    return jnp.where((block_of(source) == one_side) | (block_of(source) == other_side), factor * entries, entries)


def steps_of(key, dims, shards, smallest, largest):
    level = 1.0
    for axis_at, parts in shards:
        heights = jax.random.uniform(jax.random.fold_in(jax.random.fold_in(key, 6), axis_at), (parts,), jnp.float32, smallest / len(shards), largest / len(shards))
        level = level * jnp.repeat(jnp.exp(heights), dims[axis_at] // parts).reshape((-1,) + (1,) * (len(dims) - 1 - axis_at))
    return level


def bell_draw(key, dims, spread, reach, cuts=(), held_as=jnp.bfloat16):
    loudness = steps_of(key, dims, cuts, -0.22, 0.18) if cuts else 1.0
    entries = jax.random.normal(key, dims, jnp.float32) * spread * loudness
    return jnp.minimum(jnp.maximum(entries, -reach), reach).astype(held_as)


def bell_draw_with(key, dims, scale, reach, cuts, heavy, kind=jnp.bfloat16):
    drawn = scale * jax.random.normal(key, dims, jnp.float32)
    if cuts:
        drawn = drawn * steps_of(key, dims, cuts, -0.22, 0.18)
    return jnp.clip(with_spikes(drawn, jax.random.fold_in(key, 3), *heavy), -reach, reach).astype(kind)


def setup_inputs(seed: int = 0, part: int = 0) -> dict:
    seeds = jax.random.split(jax.random.key(seed), 8)
    part_splits = jax.random.split(jax.random.fold_in(seeds[7], part), 8)
    return {
        "tokens": bell_draw(part_splits[0], (SEQ, SEQS, D), 1.0, 6.0, ((0, 32),)),
        "w_query": draw_w_query(jax.random.fold_in(seeds[7], 71), part),
        "w_key": draw_w_key(jax.random.fold_in(seeds[7], 71), part),
        "w_value": bell_draw(seeds[3], (D, HEADS * HEAD_DIM), D ** -0.5, 0.078125, ((1, 4),)),
        "w_out": bell_draw_with(seeds[4], (HEADS * HEAD_DIM, D), (HEADS * HEAD_DIM) ** -0.5, 0.125, ((0, 4),), (0, 1, 4, 2.0)),
        "gain_query": draw_gain_query(jax.random.fold_in(seeds[7], 71), part),
        "gain_key": draw_gain_key(jax.random.fold_in(seeds[7], 71), part),
    }


def rotary(field, positions):
    half = HEAD_DIM // 2
    shaped = field.reshape(field.shape[0], -1, HEAD_DIM)
    freqs = jnp.exp(-jnp.log(500000.0) * jnp.arange(half, dtype=jnp.float32) * 2.0 / HEAD_DIM)
    angle = positions.astype(jnp.float32)[:, None] * freqs[None, :]
    cosine = jnp.cos(angle)[:, None, :]
    sine = jnp.sin(angle)[:, None, :]
    first = shaped[..., :half]
    second = shaped[..., half:]
    turned = jnp.concatenate([first * cosine - second * sine, second * cosine + first * sine], axis=-1)
    return turned.reshape(field.shape[0], -1)

def one_sequence(seq_tokens, w_query, w_key, w_value, w_out, gain_query, gain_key):
    width = HEADS * HEAD_DIM
    query = jnp.dot(seq_tokens, w_query, preferred_element_type=jnp.float32)
    key_raw = jnp.dot(seq_tokens, w_key, preferred_element_type=jnp.float32)
    value = jnp.dot(seq_tokens, w_value, preferred_element_type=jnp.float32).astype(jnp.bfloat16)
    scale_q = lax.rsqrt(lax.optimization_barrier(jnp.sum(query * query, axis=1)) / width + 1e-06)
    scale_k = lax.rsqrt(lax.optimization_barrier(jnp.sum(key_raw * key_raw, axis=1)) / width + 1e-06)
    positions = jnp.arange(SEQ, dtype=jnp.int32)
    q_normed = rotary(query * scale_q[:, None] * gain_query[None, :], positions).astype(jnp.bfloat16)
    k_normed = rotary(key_raw * scale_k[:, None] * gain_key[None, :], positions).astype(jnp.bfloat16)
    keys_all = k_normed.reshape(SEQ, HEADS, HEAD_DIM).astype(jnp.float32)
    values_all = value.reshape(SEQ, HEADS, HEAD_DIM).astype(jnp.float32)
    factor = HEAD_DIM ** (-0.5)

    def one_block(index):
        start = (index * TOK_DEV).astype(jnp.int32)
        q_block = lax.dynamic_slice_in_dim(q_normed, start, TOK_DEV, 0).reshape(TOK_DEV, HEADS, HEAD_DIM).astype(jnp.float32)
        scores = jnp.einsum('qhd,khd->hqk', q_block, keys_all) * factor
        q_pos = start + jnp.arange(TOK_DEV, dtype=jnp.int32)
        allowed = positions[None, None, :] <= q_pos[None, :, None]
        top = lax.optimization_barrier(jnp.max(jnp.where(allowed, scores, -1e+30), axis=2))
        expo = jnp.where(allowed, jnp.exp(scores - top[..., None]), 0.0)
        total = lax.optimization_barrier(jnp.sum(expo, axis=2))
        rounded = expo.astype(jnp.bfloat16).astype(jnp.float32)
        summed = jnp.einsum('hqk,khd->hqd', rounded, values_all)
        mixed = (summed / total[..., None]).astype(jnp.bfloat16)
        return jnp.transpose(mixed, (1, 0, 2)).reshape(TOK_DEV, width)
    blocks = lax.map(one_block, jnp.arange(SEQ // TOK_DEV, dtype=jnp.int32))
    mixed_all = blocks.reshape(SEQ, width)
    return jnp.dot(mixed_all, w_out, preferred_element_type=jnp.float32).astype(jnp.bfloat16)

def reference(tokens, w_query, w_key, w_value, w_out, gain_query, gain_key):
    by_sequence = jnp.transpose(tokens, (1, 0, 2))

    def handle(seq_tokens):
        return one_sequence(seq_tokens, w_query, w_key, w_value, w_out, gain_query, gain_key)
    results = lax.map(handle, by_sequence)
    return jnp.transpose(results, (1, 0, 2))
```

```python
import jax
import jax.numpy as jnp
from jax import lax
from jax.experimental import pallas as pl
from jax.experimental.pallas import tpu as pltpu
from jax.sharding import PartitionSpec as P

HEADS = 40
HEAD_DIM = 128
HALF = HEAD_DIM // 2
LOG2E = 1.4426950408889634
BLOCK = 256


def turn_tables(first_token, rows):
    freqs = jnp.exp(-jnp.log(500000.0) * jnp.arange(HALF, dtype=jnp.float32) * 2.0 / HEAD_DIM)
    positions = first_token + jnp.arange(rows, dtype=jnp.int32)
    angle = positions.astype(jnp.float32)[:, None] * freqs[None, :]
    cosine, sine = jnp.cos(angle), jnp.sin(angle)
    return jnp.concatenate([cosine, cosine], 1), jnp.concatenate([-sine, sine], 1)


def pack_value(value, slots, seqs, rows, heads):
    def body(v_ref, out_ref, head_ref):
        for h in range(heads):
            head_ref[h] = v_ref[:, h * HEAD_DIM : (h + 1) * HEAD_DIM]
            for j in range(seqs):
                part = head_ref[h, pl.ds(j, rows, stride=seqs), :]
                out_ref[j * heads + h] = part.astype(jnp.bfloat16)

    return pl.pallas_call(
        body,
        out_shape=jax.ShapeDtypeStruct((slots, rows, HEAD_DIM), jnp.bfloat16),
        scratch_shapes=[pltpu.VMEM((heads, seqs * rows, HEAD_DIM), jnp.float32)],
        name="pack_value",
    )(value)


def pack_query_key(query, key, scale_q, scale_k, gain_q, gain_k, cosine, sine, slots, seqs, rows, heads):
    def body(q_ref, k_ref, sq_ref, sk_ref, gq_ref, gk_ref, c_ref, s_ref, out_ref, head_ref):
        cos, sin = c_ref[...], s_ref[...]
        for which, (x_ref, r_ref, g_ref) in enumerate(((q_ref, sq_ref, gq_ref), (k_ref, sk_ref, gk_ref))):
            for h in range(heads):
                cols = slice(h * HEAD_DIM, (h + 1) * HEAD_DIM)
                head_ref[which, h] = x_ref[:, cols] * r_ref[...] * g_ref[:, cols]
                for j in range(seqs):
                    part = head_ref[which, h, pl.ds(j, rows, stride=seqs), :]
                    turned = part * cos + pltpu.roll(part, HALF, 1) * sin
                    out_ref[j * heads + h, which] = turned.astype(jnp.bfloat16)

    return pl.pallas_call(
        body,
        out_shape=jax.ShapeDtypeStruct((slots, 2, rows, HEAD_DIM), jnp.bfloat16),
        scratch_shapes=[pltpu.VMEM((2, heads, seqs * rows, HEAD_DIM), jnp.float32)],
        name="pack_query_key",
    )(query, key, scale_q, scale_k, gain_q, gain_k, cosine, sine)


def attend(query_key, value):
    blocks, rows = value.shape[0], value.shape[1]
    per = BLOCK // rows
    steps = blocks // per
    power = HEAD_DIM ** (-0.5) * LOG2E

    def body(qk_ref, v_ref, out_ref, s_ref):
        row = lax.broadcasted_iota(jnp.int32, (BLOCK, BLOCK), 0)
        col = lax.broadcasted_iota(jnp.int32, (BLOCK, BLOCK), 1)
        for i in range(steps):
            q = qk_ref[per * i : per * (i + 1), 0].reshape(BLOCK, HEAD_DIM)
            top = None
            for c in range(i + 1):
                k = qk_ref[per * c : per * (c + 1), 1].reshape(BLOCK, HEAD_DIM)
                s = lax.dot_general(q, k, (((1,), (1,)), ((), ())), preferred_element_type=jnp.float32)
                if c == i:
                    s = jnp.where(col <= row, s, -1e30)
                s_ref[:, c * BLOCK : (c + 1) * BLOCK] = s
                best = jnp.maximum(s[:, :HEAD_DIM], s[:, HEAD_DIM:])
                top = best if top is None else jnp.maximum(top, best)
            top = jnp.max(top, axis=1, keepdims=True)
            total = jnp.zeros((BLOCK, HEAD_DIM), jnp.float32)
            acc = jnp.zeros((BLOCK, HEAD_DIM), jnp.float32)
            for c in range(i + 1):
                e = jnp.exp2((s_ref[:, c * BLOCK : (c + 1) * BLOCK] - top) * power)
                total = total + e[:, :HEAD_DIM] + e[:, HEAD_DIM:]
                v = v_ref[per * c : per * (c + 1)].reshape(BLOCK, HEAD_DIM)
                acc = acc + jnp.dot(e.astype(jnp.bfloat16), v, preferred_element_type=jnp.float32)
            mixed = acc / jnp.sum(total, axis=1, keepdims=True)
            out_ref[per * i : per * (i + 1)] = mixed.astype(jnp.bfloat16).reshape(per, rows, HEAD_DIM)

    return pl.pallas_call(
        body,
        out_shape=jax.ShapeDtypeStruct((blocks, rows, HEAD_DIM), jnp.bfloat16),
        scratch_shapes=[pltpu.VMEM((BLOCK, blocks * rows), jnp.float32)],
        name="attend",
    )(query_key, value)


def unpack_mixed(parts, seqs, heads):
    rows = parts.shape[1]

    def body(in_ref, out_ref, head_ref):
        for h in range(heads):
            for j in range(seqs):
                head_ref[h, pl.ds(j, rows, stride=seqs), :] = in_ref[j * heads + h].astype(jnp.float32)
            out_ref[:, h * HEAD_DIM : (h + 1) * HEAD_DIM] = head_ref[h].astype(jnp.bfloat16)

    return pl.pallas_call(
        body,
        out_shape=jax.ShapeDtypeStruct((rows * seqs, heads * HEAD_DIM), jnp.bfloat16),
        scratch_shapes=[pltpu.VMEM((heads, rows * seqs, HEAD_DIM), jnp.float32)],
        name="unpack_mixed",
    )(parts)


def exchange(array, axis):
    return lax.all_to_all(array, axis, 0, 0, tiled=True)


def local(tokens, w_query, w_key, w_value, w_out, gain_query, gain_key):
    rows, seqs, depth = tokens.shape
    local_width = w_query.shape[1]
    heads = local_width // HEAD_DIM
    width = HEADS * HEAD_DIM
    slots = lax.axis_size("seq")
    flat = tokens.reshape(rows * seqs, depth)
    cosine, sine = turn_tables(lax.axis_index("seq") * rows, rows)

    value = jnp.dot(flat, w_value, preferred_element_type=jnp.float32)
    sent_v = pack_value(value, slots, seqs, rows, heads)
    flat, sent_v = lax.optimization_barrier((flat, sent_v))
    got_v = exchange(sent_v, "seq")

    query = jnp.dot(flat, w_query, preferred_element_type=jnp.float32)
    key_raw = jnp.dot(flat, w_key, preferred_element_type=jnp.float32)
    squares = jnp.concatenate([jnp.sum(query * query, axis=1), jnp.sum(key_raw * key_raw, axis=1)])
    everyone = jnp.broadcast_to(squares, (lax.axis_size("tensor"), *squares.shape))
    sums = jnp.sum(exchange(everyone, "tensor"), axis=0)
    scales = lax.rsqrt(sums / width + 1e-06)
    lanes = jnp.broadcast_to(scales[:, None], (scales.shape[0], HEAD_DIM))
    sent_qk = pack_query_key(
        query, key_raw, lanes[: rows * seqs], lanes[rows * seqs :], gain_query[None, :], gain_key[None, :],
        cosine, sine, slots, seqs, rows, heads,
    )
    got_qk = exchange(sent_qk, "seq")

    mixed = exchange(attend(got_qk, got_v), "seq")
    flat_mixed = unpack_mixed(mixed[: seqs * heads], seqs, heads)
    partial = jnp.dot(flat_mixed, w_out, preferred_element_type=jnp.float32).astype(jnp.bfloat16)
    pieces = exchange(partial.reshape(lax.axis_size("tensor"), -1, depth), "tensor")
    attended = jnp.sum(pieces.astype(jnp.float32), axis=0).astype(jnp.bfloat16)
    return attended.reshape(-1, seqs, depth)


def solution(mesh):
    return jax.shard_map(
        local,
        mesh=mesh,
        in_specs=(
            P("seq", "dp", None),
            P(None, "tensor"),
            P(None, "tensor"),
            P(None, "tensor"),
            P("tensor", None),
            P("tensor"),
            P("tensor"),
        ),
        out_specs=P(("seq", "tensor"), "dp", None),
        check_vma=False,
    )
```

```python
import jax
import jax.numpy as jnp
from jax import lax
from jax.experimental import pallas as pl
from jax.experimental.pallas import tpu as pltpu
from jax.sharding import PartitionSpec as P


HEADS = 40
HEAD_DIM = 128
HALF = HEAD_DIM // 2
LOG2E = 1.4426950408889634
BLOCK = 256
AHEAD = 4
ROWS_IN = 512


def row_of(column):
    return jnp.sum(column.T, axis=0, keepdims=True)


def stream(x_ref, weights, sums, buffer, arrived, before):
    block = buffer.shape[1]
    blocks = weights[0].shape[0] // block

    def copy(which, n):
        at = (which * blocks + n) % (AHEAD + 1)
        return pltpu.make_async_copy(weights[which].at[pl.ds(n * block, block), :], buffer.at[at], arrived.at[at])

    for n in range(AHEAD):
        copy(0, n).start()
    before()
    for which in range(len(weights)):

        def step(n, _, which=which):
            @pl.when(n + AHEAD < blocks)
            def _():
                copy(which, n + AHEAD).start()

            if which + 1 < len(weights):

                @pl.when(n + AHEAD >= blocks)
                def _():
                    copy(which + 1, n + AHEAD - blocks).start()

            copy(which, n).wait()
            columns = pl.ds(pl.multiple_of(n * block, block), block)
            part = buffer[(which * blocks + n) % (AHEAD + 1)]
            sums[which][...] += jnp.dot(x_ref[:, columns], part, preferred_element_type=jnp.float32)
            return 0

        sums[which][...] = jnp.zeros_like(sums[which])
        lax.fori_loop(0, blocks, step, 0)


def project_value(tokens, weight, slots):
    rows, seqs, depth = tokens.shape
    total, width = rows * seqs, weight.shape[1]
    heads = width // HEAD_DIM

    def body(in_ref, w_ref, x_ref, out_ref, sums, buffer, arrived, head_ref, token_ref, here):
        tokens_in = pltpu.make_async_copy(in_ref, token_ref, here)
        tokens_in.start()

        def before():
            tokens_in.wait()
            x_ref[...] = token_ref[...].reshape(total, depth)

        stream(x_ref, (w_ref,), (sums,), buffer, arrived, before)
        for h in range(heads):
            head_ref[h] = sums[:, h * HEAD_DIM : (h + 1) * HEAD_DIM]
            for j in range(seqs):
                out_ref[j * heads + h] = head_ref[h, pl.ds(j, rows, stride=seqs), :].astype(jnp.bfloat16)

    vmem = pl.BlockSpec(memory_space=pltpu.VMEM)
    return pl.pallas_call(
        body,
        in_specs=[pl.BlockSpec(memory_space=pltpu.HBM)] * 2,
        out_specs=[vmem, vmem],
        out_shape=[
            jax.ShapeDtypeStruct((total, depth), jnp.bfloat16),
            jax.ShapeDtypeStruct((slots, rows, HEAD_DIM), jnp.bfloat16),
        ],
        scratch_shapes=[
            pltpu.VMEM((total, width), jnp.float32),
            pltpu.VMEM((AHEAD + 1, ROWS_IN, width), jnp.bfloat16),
            pltpu.SemaphoreType.DMA((AHEAD + 1,)),
            pltpu.VMEM((heads, total, HEAD_DIM), jnp.float32),
            pltpu.VMEM(tokens.shape, jnp.bfloat16),
            pltpu.SemaphoreType.DMA,
        ],
        compiler_params=pltpu.CompilerParams(vmem_limit_bytes=53 << 20),
        name="project_value",
    )(tokens, weight)


def turn_tables(first_token, rows):
    def body(at_ref, c_ref, s_ref):
        lane = lax.broadcasted_iota(jnp.int32, (rows, HEAD_DIM), 1)
        token = at_ref[0] + lax.broadcasted_iota(jnp.int32, (rows, HEAD_DIM), 0)
        pair = jnp.where(lane < HALF, lane, lane - HALF).astype(jnp.float32)
        angle = token.astype(jnp.float32) * jnp.exp(-jnp.log(500000.0) * pair * 2.0 / HEAD_DIM)
        c_ref[...] = jnp.cos(angle)
        s_ref[...] = jnp.where(lane < HALF, -jnp.sin(angle), jnp.sin(angle))

    return pl.pallas_call(
        body,
        in_specs=[pl.BlockSpec(memory_space=pltpu.SMEM)],
        out_shape=[jax.ShapeDtypeStruct((rows, HEAD_DIM), jnp.float32)] * 2,
        compiler_params=pltpu.CompilerParams(vmem_limit_bytes=4 << 20),
        name="turn_tables",
    )(first_token)


def project_query_key(flat, w_query, w_key):
    total, _ = flat.shape
    heads = w_query.shape[1] // HEAD_DIM

    def body(x_ref, wq_ref, wk_ref, q_ref, k_ref, sums_ref, sums, buffer, arrived):
        stream(x_ref, (wq_ref, wk_ref), (sums.at[0], sums.at[1]), buffer, arrived, lambda: None)
        squares = []
        for which, out_ref in enumerate((q_ref, k_ref)):
            square = jnp.zeros((total, HEAD_DIM), jnp.float32)
            for h in range(heads):
                part = sums[which, :, h * HEAD_DIM : (h + 1) * HEAD_DIM]
                out_ref[h] = part
                square = square + part * part
            squares.append(row_of(square))
        sums_ref[...] = jnp.concatenate(squares * 4, axis=0)

    vmem, hbm = pl.BlockSpec(memory_space=pltpu.VMEM), pl.BlockSpec(memory_space=pltpu.HBM)
    return pl.pallas_call(
        body,
        in_specs=[vmem, hbm, hbm],
        out_specs=[vmem] * 3,
        out_shape=[
            jax.ShapeDtypeStruct((heads, total, HEAD_DIM), jnp.float32),
            jax.ShapeDtypeStruct((heads, total, HEAD_DIM), jnp.float32),
            jax.ShapeDtypeStruct((8, total), jnp.float32),
        ],
        scratch_shapes=[
            pltpu.VMEM((2, total, heads * HEAD_DIM), jnp.float32),
            pltpu.VMEM((AHEAD + 1, ROWS_IN, heads * HEAD_DIM), jnp.bfloat16),
            pltpu.SemaphoreType.DMA((AHEAD + 1,)),
        ],
        compiler_params=pltpu.CompilerParams(vmem_limit_bytes=53 << 20),
        name="project_query_key",
    )(flat, w_query, w_key)


def pack(query, key, sums, gains, cosine, sine, slots, seqs):
    heads, total, _ = query.shape
    rows, width = total // seqs, HEADS * HEAD_DIM

    def body(q_ref, k_ref, sums_ref, g_ref, c_ref, s_ref, out_ref, row_ref, head_ref):
        cos, sin = c_ref[...], s_ref[...]
        everyone = sums_ref[0]
        for other in range(1, sums_ref.shape[0]):
            everyone = everyone + sums_ref[other]
        scale = lax.rsqrt(everyone / width + 1e-06)
        for which, x_ref in enumerate((q_ref, k_ref)):
            row_ref[...] = jnp.broadcast_to(scale[which : which + 1, :], (HEAD_DIM, total)).T
            for h in range(heads):
                head_ref[h] = x_ref[h] * row_ref[...] * g_ref[which, h : h + 1, :]
                for j in range(seqs):
                    part = head_ref[h, pl.ds(j, rows, stride=seqs), :]
                    turned = part * cos + pltpu.roll(part, HALF, 1) * sin
                    out_ref[j * heads + h, which] = turned.astype(jnp.bfloat16)

    return pl.pallas_call(
        body,
        out_shape=jax.ShapeDtypeStruct((slots, 2, rows, HEAD_DIM), jnp.bfloat16),
        scratch_shapes=[
            pltpu.VMEM((total, HEAD_DIM), jnp.float32),
            pltpu.VMEM((heads, total, HEAD_DIM), jnp.float32),
        ],
        compiler_params=pltpu.CompilerParams(vmem_limit_bytes=16 << 20),
        name="pack",
    )(query, key, sums, gains, cosine, sine)


def attend(query_key, value):
    blocks, rows, _ = value.shape
    per = BLOCK // rows
    steps = blocks // per
    power = HEAD_DIM ** (-0.5) * LOG2E

    def body(in_ref, v_ref, out_ref, s_ref):
        row = lax.broadcasted_iota(jnp.int32, (BLOCK, BLOCK), 0)
        col = lax.broadcasted_iota(jnp.int32, (BLOCK, BLOCK), 1)
        for i in range(steps):
            q = in_ref[per * i : per * (i + 1), 0].reshape(BLOCK, HEAD_DIM)
            top = None
            for c in range(i + 1):
                k = in_ref[per * c : per * (c + 1), 1].reshape(BLOCK, HEAD_DIM)
                s = lax.dot_general(q, k, (((1,), (1,)), ((), ())), preferred_element_type=jnp.float32)
                if c == i:
                    s = jnp.where(col <= row, s, -1e30)
                s_ref[:, c * BLOCK : (c + 1) * BLOCK] = s
                best = jnp.maximum(s[:, :HEAD_DIM], s[:, HEAD_DIM:])
                top = best if top is None else jnp.maximum(top, best)
            top = jnp.max(top, axis=1, keepdims=True)
            total = jnp.zeros((BLOCK, HEAD_DIM), jnp.float32)
            acc = jnp.zeros((BLOCK, HEAD_DIM), jnp.float32)
            for c in range(i + 1):
                e = jnp.exp2((s_ref[:, c * BLOCK : (c + 1) * BLOCK] - top) * power)
                total = total + e[:, :HEAD_DIM] + e[:, HEAD_DIM:]
                v = v_ref[per * c : per * (c + 1)].reshape(BLOCK, HEAD_DIM)
                acc = acc + jnp.dot(e.astype(jnp.bfloat16), v, preferred_element_type=jnp.float32)
            mixed = acc / jnp.sum(total, axis=1, keepdims=True)
            out_ref[per * i : per * (i + 1)] = mixed.astype(jnp.bfloat16).reshape(per, rows, HEAD_DIM)

    return pl.pallas_call(
        body,
        out_shape=jax.ShapeDtypeStruct((blocks, rows, HEAD_DIM), jnp.bfloat16),
        scratch_shapes=[pltpu.VMEM((BLOCK, blocks * rows), jnp.float32)],
        compiler_params=pltpu.CompilerParams(vmem_limit_bytes=16 << 20),
        cost_estimate=pl.CostEstimate(
            flops=64 * (blocks * rows) ** 2 * HEAD_DIM,
            transcendentals=(blocks * rows) ** 2 // 2,
            bytes_accessed=8 * blocks * rows * HEAD_DIM,
        ),
        name="attend",
    )(query_key, value)


def project_out(parts, weight, seqs):
    rows = parts.shape[1]
    local_width, depth = weight.shape
    heads = local_width // HEAD_DIM
    wide = 512

    def body(in_ref, w_ref, out_ref, head_ref, x_ref):
        for h in range(heads):
            for j in range(seqs):
                head_ref[h, pl.ds(j, rows, stride=seqs), :] = in_ref[j * heads + h].astype(jnp.float32)
            x_ref[:, h * HEAD_DIM : (h + 1) * HEAD_DIM] = head_ref[h].astype(jnp.bfloat16)

        def step(n, _):
            columns = pl.ds(pl.multiple_of(n * wide, wide), wide)
            got = jnp.dot(x_ref[...], w_ref[:, columns], preferred_element_type=jnp.float32)
            out_ref[:, columns] = got.astype(jnp.bfloat16)
            return 0

        lax.fori_loop(0, depth // wide, step, 0)

    vmem = pl.BlockSpec(memory_space=pltpu.VMEM)
    return pl.pallas_call(
        body,
        in_specs=[vmem, vmem],
        out_specs=vmem,
        out_shape=jax.ShapeDtypeStruct((rows * seqs, depth), jnp.bfloat16),
        scratch_shapes=[
            pltpu.VMEM((heads, rows * seqs, HEAD_DIM), jnp.float32),
            pltpu.VMEM((rows * seqs, local_width), jnp.bfloat16),
        ],
        compiler_params=pltpu.CompilerParams(vmem_limit_bytes=8 << 20),
        cost_estimate=pl.CostEstimate(
            flops=2 * rows * seqs * local_width * depth, transcendentals=0, bytes_accessed=2 * local_width * depth
        ),
        name="project_out",
    )(parts, weight)


def exchange(array, axis):
    return lax.all_to_all(array, axis, 0, 0, tiled=True)


def local(tokens, w_query, w_key, w_value, w_out, gain_query, gain_key):
    rows, seqs, depth = tokens.shape
    heads = w_query.shape[1] // HEAD_DIM
    slots, fold = lax.axis_size("seq"), lax.axis_size("tensor")
    first_token = (lax.axis_index("seq") * rows).astype(jnp.int32)[None]
    gains = jnp.stack([gain_query, gain_key]).reshape(2, heads, HEAD_DIM)

    flat, sent_v = project_value(tokens, w_value, slots)
    got_v = exchange(sent_v, "seq")
    query, key_raw, squares = project_query_key(flat, w_query, w_key)
    cosine, sine = turn_tables(first_token, rows)
    others = [
        lax.ppermute(squares, "tensor", [(i, (i + shift) % fold) for i in range(fold)])
        for shift in range(1, fold)
    ]
    sent_qk = pack(query, key_raw, jnp.stack([squares, *others]), gains, cosine, sine, slots, seqs)
    mixed = exchange(attend(exchange(sent_qk, "seq"), got_v), "seq")
    partial = project_out(mixed, w_out, seqs)
    pieces = exchange(partial.reshape(fold, -1, depth), "tensor")
    attended = jnp.sum(pieces.astype(jnp.float32), axis=0).astype(jnp.bfloat16)
    return attended.reshape(-1, seqs, depth)


def solution(mesh):
    return jax.shard_map(
        local,
        mesh=mesh,
        in_specs=(
            P("seq", "dp", None),
            P(None, "tensor"),
            P(None, "tensor"),
            P(None, "tensor"),
            P("tensor", None),
            P("tensor"),
            P("tensor"),
        ),
        out_specs=P(("seq", "tensor"), "dp", None),
        check_vma=False,
    )
```

```python
import jax
import jax.numpy as jnp
from jax import lax
from jax.experimental import pallas as pl
from jax.experimental.pallas import tpu as pltpu
from jax.sharding import PartitionSpec as P


HEADS = 40
HEAD_DIM = 128
HALF = HEAD_DIM // 2
LOG2E = 1.4426950408889634
BLOCK = 256
AHEAD = 4
ROWS_IN = 512


def row_of(column):
    return jnp.sum(column.T, axis=0, keepdims=True)


def in_hbm(array):
    return pltpu.with_memory_space_constraint(array, pltpu.HBM)


def stream(x_ref, weights, sums, buffer, arrived, before):
    block = buffer.shape[1]
    blocks = weights[0].shape[0] // block

    def copy(which, n):
        at = (which * blocks + n) % (AHEAD + 1)
        return pltpu.make_async_copy(weights[which].at[pl.ds(n * block, block), :], buffer.at[at], arrived.at[at])

    for n in range(AHEAD):
        copy(0, n).start()
    before()
    for which in range(len(weights)):

        def step(n, _, which=which):
            @pl.when(n + AHEAD < blocks)
            def _():
                copy(which, n + AHEAD).start()

            if which + 1 < len(weights):

                @pl.when(n + AHEAD >= blocks)
                def _():
                    copy(which + 1, n + AHEAD - blocks).start()

            copy(which, n).wait()
            columns = pl.ds(pl.multiple_of(n * block, block), block)
            part = buffer[(which * blocks + n) % (AHEAD + 1)]
            sums[which][...] += jnp.dot(x_ref[:, columns], part, preferred_element_type=jnp.float32)
            return 0

        sums[which][...] = jnp.zeros_like(sums[which])
        lax.fori_loop(0, blocks, step, 0)


def project_value(tokens, weight, slots):
    rows, seqs, depth = tokens.shape
    total, width = rows * seqs, weight.shape[1]
    heads = width // HEAD_DIM

    def body(in_ref, w_ref, x_ref, out_ref, sums, buffer, arrived, head_ref, token_ref, here):
        tokens_in = pltpu.make_async_copy(in_ref, token_ref, here)
        tokens_in.start()

        def before():
            tokens_in.wait()
            x_ref[...] = token_ref[...].reshape(total, depth)

        stream(x_ref, (w_ref,), (sums,), buffer, arrived, before)
        for h in range(heads):
            head_ref[h] = sums[:, h * HEAD_DIM : (h + 1) * HEAD_DIM]
            for j in range(seqs):
                out_ref[j * heads + h] = head_ref[h, pl.ds(j, rows, stride=seqs), :].astype(jnp.bfloat16)

    vmem = pl.BlockSpec(memory_space=pltpu.VMEM)
    return pl.pallas_call(
        body,
        in_specs=[pl.BlockSpec(memory_space=pltpu.HBM)] * 2,
        out_specs=[vmem, vmem],
        out_shape=[
            jax.ShapeDtypeStruct((total, depth), jnp.bfloat16),
            jax.ShapeDtypeStruct((slots, rows, HEAD_DIM), jnp.bfloat16),
        ],
        scratch_shapes=[
            pltpu.VMEM((total, width), jnp.float32),
            pltpu.VMEM((AHEAD + 1, ROWS_IN, width), jnp.bfloat16),
            pltpu.SemaphoreType.DMA((AHEAD + 1,)),
            pltpu.VMEM((heads, total, HEAD_DIM), jnp.float32),
            pltpu.VMEM(tokens.shape, jnp.bfloat16),
            pltpu.SemaphoreType.DMA,
        ],
        compiler_params=pltpu.CompilerParams(vmem_limit_bytes=24 << 20),
        name="project_value",
    )(in_hbm(tokens), in_hbm(weight))


def turn_tables(first_token, rows):
    def body(at_ref, c_ref, s_ref):
        lane = lax.broadcasted_iota(jnp.int32, (rows, HEAD_DIM), 1)
        token = at_ref[0] + lax.broadcasted_iota(jnp.int32, (rows, HEAD_DIM), 0)
        pair = jnp.where(lane < HALF, lane, lane - HALF).astype(jnp.float32)
        angle = token.astype(jnp.float32) * jnp.exp(-jnp.log(500000.0) * pair * 2.0 / HEAD_DIM)
        c_ref[...] = jnp.cos(angle)
        s_ref[...] = jnp.where(lane < HALF, -jnp.sin(angle), jnp.sin(angle))

    return pl.pallas_call(
        body,
        in_specs=[pl.BlockSpec(memory_space=pltpu.SMEM)],
        out_shape=[jax.ShapeDtypeStruct((rows, HEAD_DIM), jnp.float32)] * 2,
        compiler_params=pltpu.CompilerParams(vmem_limit_bytes=4 << 20),
        name="turn_tables",
    )(first_token)


def project_query_key(flat, w_query, w_key):
    total, _ = flat.shape
    heads = w_query.shape[1] // HEAD_DIM

    def body(x_ref, wq_ref, wk_ref, q_ref, k_ref, sums_ref, sums, buffer, arrived):
        stream(x_ref, (wq_ref, wk_ref), (sums.at[0], sums.at[1]), buffer, arrived, lambda: None)
        squares = []
        for which, out_ref in enumerate((q_ref, k_ref)):
            square = jnp.zeros((total, HEAD_DIM), jnp.float32)
            for h in range(heads):
                part = sums[which, :, h * HEAD_DIM : (h + 1) * HEAD_DIM]
                out_ref[h] = part
                square = square + part * part
            squares.append(row_of(square))
        sums_ref[...] = jnp.concatenate(squares * 4, axis=0)

    vmem, hbm = pl.BlockSpec(memory_space=pltpu.VMEM), pl.BlockSpec(memory_space=pltpu.HBM)
    return pl.pallas_call(
        body,
        in_specs=[vmem, hbm, hbm],
        out_specs=[vmem] * 3,
        out_shape=[
            jax.ShapeDtypeStruct((heads, total, HEAD_DIM), jnp.float32),
            jax.ShapeDtypeStruct((heads, total, HEAD_DIM), jnp.float32),
            jax.ShapeDtypeStruct((8, total), jnp.float32),
        ],
        scratch_shapes=[
            pltpu.VMEM((2, total, heads * HEAD_DIM), jnp.float32),
            pltpu.VMEM((AHEAD + 1, ROWS_IN, heads * HEAD_DIM), jnp.bfloat16),
            pltpu.SemaphoreType.DMA((AHEAD + 1,)),
        ],
        compiler_params=pltpu.CompilerParams(vmem_limit_bytes=24 << 20),
        name="project_query_key",
    )(flat, in_hbm(w_query), in_hbm(w_key))


def pack(query, key, sums, gains, cosine, sine, slots, seqs):
    heads, total, _ = query.shape
    rows, width = total // seqs, HEADS * HEAD_DIM

    def body(q_ref, k_ref, sums_ref, g_ref, c_ref, s_ref, out_ref, row_ref, head_ref):
        cos, sin = c_ref[...], s_ref[...]
        everyone = sums_ref[0]
        for other in range(1, sums_ref.shape[0]):
            everyone = everyone + sums_ref[other]
        scale = lax.rsqrt(everyone / width + 1e-06)
        for which, x_ref in enumerate((q_ref, k_ref)):
            row_ref[...] = jnp.broadcast_to(scale[which : which + 1, :], (HEAD_DIM, total)).T
            for h in range(heads):
                head_ref[h] = x_ref[h] * row_ref[...] * g_ref[which, h : h + 1, :]
                for j in range(seqs):
                    part = head_ref[h, pl.ds(j, rows, stride=seqs), :]
                    turned = part * cos + pltpu.roll(part, HALF, 1) * sin
                    out_ref[j * heads + h, which] = turned.astype(jnp.bfloat16)

    return pl.pallas_call(
        body,
        out_shape=jax.ShapeDtypeStruct((slots, 2, rows, HEAD_DIM), jnp.bfloat16),
        scratch_shapes=[
            pltpu.VMEM((total, HEAD_DIM), jnp.float32),
            pltpu.VMEM((heads, total, HEAD_DIM), jnp.float32),
        ],
        compiler_params=pltpu.CompilerParams(vmem_limit_bytes=16 << 20),
        name="pack",
    )(query, key, sums, gains, cosine, sine)


def attend(query_key, value):
    blocks, rows, _ = value.shape
    per = BLOCK // rows
    steps = blocks // per
    power = HEAD_DIM ** (-0.5) * LOG2E

    def body(in_ref, v_ref, out_ref, s_ref):
        row = lax.broadcasted_iota(jnp.int32, (BLOCK, BLOCK), 0)
        col = lax.broadcasted_iota(jnp.int32, (BLOCK, BLOCK), 1)
        for i in range(steps):
            q = in_ref[per * i : per * (i + 1), 0].reshape(BLOCK, HEAD_DIM)
            top = None
            for c in range(i + 1):
                k = in_ref[per * c : per * (c + 1), 1].reshape(BLOCK, HEAD_DIM)
                s = lax.dot_general(q, k, (((1,), (1,)), ((), ())), preferred_element_type=jnp.float32)
                if c == i:
                    s = jnp.where(col <= row, s, -1e30)
                s_ref[:, c * BLOCK : (c + 1) * BLOCK] = s
                best = jnp.maximum(s[:, :HEAD_DIM], s[:, HEAD_DIM:])
                top = best if top is None else jnp.maximum(top, best)
            top = jnp.max(top, axis=1, keepdims=True)
            total = jnp.zeros((BLOCK, HEAD_DIM), jnp.float32)
            acc = jnp.zeros((BLOCK, HEAD_DIM), jnp.float32)
            for c in range(i + 1):
                e = jnp.exp2((s_ref[:, c * BLOCK : (c + 1) * BLOCK] - top) * power)
                total = total + e[:, :HEAD_DIM] + e[:, HEAD_DIM:]
                v = v_ref[per * c : per * (c + 1)].reshape(BLOCK, HEAD_DIM)
                acc = acc + jnp.dot(e.astype(jnp.bfloat16), v, preferred_element_type=jnp.float32)
            mixed = acc / jnp.sum(total, axis=1, keepdims=True)
            out_ref[per * i : per * (i + 1)] = mixed.astype(jnp.bfloat16).reshape(per, rows, HEAD_DIM)

    return pl.pallas_call(
        body,
        out_shape=jax.ShapeDtypeStruct((blocks, rows, HEAD_DIM), jnp.bfloat16),
        scratch_shapes=[pltpu.VMEM((BLOCK, blocks * rows), jnp.float32)],
        compiler_params=pltpu.CompilerParams(vmem_limit_bytes=16 << 20),
        cost_estimate=pl.CostEstimate(
            flops=64 * (blocks * rows) ** 2 * HEAD_DIM,
            transcendentals=(blocks * rows) ** 2 // 2,
            bytes_accessed=8 * blocks * rows * HEAD_DIM,
        ),
        name="attend",
    )(query_key, value)


def project_out(parts, weight, seqs):
    rows = parts.shape[1]
    local_width, depth = weight.shape
    heads = local_width // HEAD_DIM
    wide = 512

    def body(in_ref, w_ref, out_ref, head_ref, x_ref):
        for h in range(heads):
            for j in range(seqs):
                head_ref[h, pl.ds(j, rows, stride=seqs), :] = in_ref[j * heads + h].astype(jnp.float32)
            x_ref[:, h * HEAD_DIM : (h + 1) * HEAD_DIM] = head_ref[h].astype(jnp.bfloat16)

        def step(n, _):
            columns = pl.ds(pl.multiple_of(n * wide, wide), wide)
            got = jnp.dot(x_ref[...], w_ref[:, columns], preferred_element_type=jnp.float32)
            out_ref[:, columns] = got.astype(jnp.bfloat16)
            return 0

        lax.fori_loop(0, depth // wide, step, 0)

    vmem = pl.BlockSpec(memory_space=pltpu.VMEM)
    return pl.pallas_call(
        body,
        in_specs=[vmem, vmem],
        out_specs=vmem,
        out_shape=jax.ShapeDtypeStruct((rows * seqs, depth), jnp.bfloat16),
        scratch_shapes=[
            pltpu.VMEM((heads, rows * seqs, HEAD_DIM), jnp.float32),
            pltpu.VMEM((rows * seqs, local_width), jnp.bfloat16),
        ],
        compiler_params=pltpu.CompilerParams(vmem_limit_bytes=8 << 20),
        cost_estimate=pl.CostEstimate(
            flops=2 * rows * seqs * local_width * depth, transcendentals=0, bytes_accessed=2 * local_width * depth
        ),
        name="project_out",
    )(parts, weight)


def exchange(array, axis):
    return lax.all_to_all(array, axis, 0, 0, tiled=True)


def local(tokens, w_query, w_key, w_value, w_out, gain_query, gain_key):
    rows, seqs, depth = tokens.shape
    heads = w_query.shape[1] // HEAD_DIM
    slots, fold = lax.axis_size("seq"), lax.axis_size("tensor")
    first_token = (lax.axis_index("seq") * rows).astype(jnp.int32)[None]
    gains = jnp.stack([gain_query, gain_key]).reshape(2, heads, HEAD_DIM)

    flat, sent_v = project_value(tokens, w_value, slots)
    got_v = exchange(sent_v, "seq")
    query, key_raw, squares = project_query_key(flat, w_query, w_key)
    cosine, sine = turn_tables(first_token, rows)
    others = [
        lax.ppermute(squares, "tensor", [(i, (i + shift) % fold) for i in range(fold)])
        for shift in range(1, fold)
    ]
    sent_qk = pack(query, key_raw, jnp.stack([squares, *others]), gains, cosine, sine, slots, seqs)
    mixed = exchange(attend(exchange(sent_qk, "seq"), got_v), "seq")
    partial = project_out(mixed, w_out, seqs)
    pieces = exchange(partial.reshape(fold, -1, depth), "tensor")
    attended = jnp.sum(pieces.astype(jnp.float32), axis=0).astype(jnp.bfloat16)
    return attended.reshape(-1, seqs, depth)


def solution(mesh):
    return jax.shard_map(
        local,
        mesh=mesh,
        in_specs=(
            P("seq", "dp", None),
            P(None, "tensor"),
            P(None, "tensor"),
            P(None, "tensor"),
            P("tensor", None),
            P("tensor"),
            P("tensor"),
        ),
        out_specs=P(("seq", "tensor"), "dp", None),
        check_vma=False,
    )
```

```python
import jax
import jax.numpy as jnp
from jax import lax
from jax.experimental import pallas as pl
from jax.experimental.pallas import tpu as pltpu
from jax.sharding import PartitionSpec as P


HEADS = 40
HEAD_DIM = 128
HALF = HEAD_DIM // 2
LOG2E = 1.4426950408889634
BLOCK = 256
AHEAD = 4
ROWS_IN = 512


def row_of(column):
    return jnp.sum(column.T, axis=0, keepdims=True)


def in_hbm(array):
    return pltpu.with_memory_space_constraint(array, pltpu.HBM)


def stream(x_ref, weights, sums, buffer, arrived, before, beside):
    block = buffer.shape[1]
    blocks = weights[0].shape[0] // block

    def copy(which, n):
        at = (which * blocks + n) % (AHEAD + 1)
        return pltpu.make_async_copy(weights[which].at[pl.ds(n * block, block), :], buffer.at[at], arrived.at[at])

    for n in range(AHEAD):
        copy(0, n).start()
    before()
    for which in range(len(weights)):

        def step(n, _, which=which):
            @pl.when(n + AHEAD < blocks)
            def _():
                copy(which, n + AHEAD).start()

            if which + 1 < len(weights):

                @pl.when(n + AHEAD >= blocks)
                def _():
                    copy(which + 1, n + AHEAD - blocks).start()

            copy(which, n).wait()
            columns = pl.ds(pl.multiple_of(n * block, block), block)
            part = buffer[(which * blocks + n) % (AHEAD + 1)]
            sums[which][...] += jnp.dot(x_ref[:, columns], part, preferred_element_type=jnp.float32)
            beside(jnp.minimum(n + 1, blocks - 1))
            return 0

        sums[which][...] = jnp.zeros_like(sums[which])
        lax.fori_loop(0, blocks, step, 0)


def project_value(tokens, weight, slots):
    rows, seqs, depth = tokens.shape
    total, width = rows * seqs, weight.shape[1]
    heads = width // HEAD_DIM

    def body(in_ref, w_ref, x_ref, out_ref, sums, buffer, arrived, head_ref, token_ref, here):
        tokens_in = pltpu.make_async_copy(in_ref, token_ref, here)
        tokens_in.start()

        def rows_of(n):
            columns = pl.ds(pl.multiple_of(n * ROWS_IN, ROWS_IN), ROWS_IN)
            x_ref[:, columns] = token_ref[:, :, columns].reshape(total, ROWS_IN)

        def before():
            tokens_in.wait()
            rows_of(0)

        stream(x_ref, (w_ref,), (sums,), buffer, arrived, before, rows_of)
        for h in range(heads):
            head_ref[h] = sums[:, h * HEAD_DIM : (h + 1) * HEAD_DIM]
            for j in range(seqs):
                out_ref[j * heads + h] = head_ref[h, pl.ds(j, rows, stride=seqs), :].astype(jnp.bfloat16)

    vmem = pl.BlockSpec(memory_space=pltpu.VMEM)
    return pl.pallas_call(
        body,
        in_specs=[pl.BlockSpec(memory_space=pltpu.HBM)] * 2,
        out_specs=[vmem, vmem],
        out_shape=[
            jax.ShapeDtypeStruct((total, depth), jnp.bfloat16),
            jax.ShapeDtypeStruct((slots, rows, HEAD_DIM), jnp.bfloat16),
        ],
        scratch_shapes=[
            pltpu.VMEM((total, width), jnp.float32),
            pltpu.VMEM((AHEAD + 1, ROWS_IN, width), jnp.bfloat16),
            pltpu.SemaphoreType.DMA((AHEAD + 1,)),
            pltpu.VMEM((heads, total, HEAD_DIM), jnp.float32),
            pltpu.VMEM(tokens.shape, jnp.bfloat16),
            pltpu.SemaphoreType.DMA,
        ],
        compiler_params=pltpu.CompilerParams(vmem_limit_bytes=24 << 20),
        name="project_value",
    )(in_hbm(tokens), in_hbm(weight))


def turn_tables(first_token, rows):
    def body(at_ref, c_ref, s_ref):
        lane = lax.broadcasted_iota(jnp.int32, (rows, HEAD_DIM), 1)
        token = at_ref[0] + lax.broadcasted_iota(jnp.int32, (rows, HEAD_DIM), 0)
        pair = jnp.where(lane < HALF, lane, lane - HALF).astype(jnp.float32)
        angle = token.astype(jnp.float32) * jnp.exp(-jnp.log(500000.0) * pair * 2.0 / HEAD_DIM)
        c_ref[...] = jnp.cos(angle)
        s_ref[...] = jnp.where(lane < HALF, -jnp.sin(angle), jnp.sin(angle))

    return pl.pallas_call(
        body,
        in_specs=[pl.BlockSpec(memory_space=pltpu.SMEM)],
        out_shape=[jax.ShapeDtypeStruct((rows, HEAD_DIM), jnp.float32)] * 2,
        compiler_params=pltpu.CompilerParams(vmem_limit_bytes=4 << 20),
        name="turn_tables",
    )(first_token)


def project_query_key(flat, w_query, w_key):
    total, _ = flat.shape
    heads = w_query.shape[1] // HEAD_DIM

    def body(x_ref, wq_ref, wk_ref, q_ref, k_ref, sums_ref, sums, buffer, arrived):
        stream(x_ref, (wq_ref, wk_ref), (sums.at[0], sums.at[1]), buffer, arrived, lambda: None, lambda n: None)
        squares = []
        for which, out_ref in enumerate((q_ref, k_ref)):
            square = jnp.zeros((total, HEAD_DIM), jnp.float32)
            for h in range(heads):
                part = sums[which, :, h * HEAD_DIM : (h + 1) * HEAD_DIM]
                out_ref[h] = part
                square = square + part * part
            squares.append(row_of(square))
        sums_ref[...] = jnp.concatenate(squares * 4, axis=0)

    vmem, hbm = pl.BlockSpec(memory_space=pltpu.VMEM), pl.BlockSpec(memory_space=pltpu.HBM)
    return pl.pallas_call(
        body,
        in_specs=[vmem, hbm, hbm],
        out_specs=[vmem] * 3,
        out_shape=[
            jax.ShapeDtypeStruct((heads, total, HEAD_DIM), jnp.float32),
            jax.ShapeDtypeStruct((heads, total, HEAD_DIM), jnp.float32),
            jax.ShapeDtypeStruct((8, total), jnp.float32),
        ],
        scratch_shapes=[
            pltpu.VMEM((2, total, heads * HEAD_DIM), jnp.float32),
            pltpu.VMEM((AHEAD + 1, ROWS_IN, heads * HEAD_DIM), jnp.bfloat16),
            pltpu.SemaphoreType.DMA((AHEAD + 1,)),
        ],
        compiler_params=pltpu.CompilerParams(vmem_limit_bytes=24 << 20),
        name="project_query_key",
    )(flat, in_hbm(w_query), in_hbm(w_key))


def pack(query, key, sums, gains, cosine, sine, slots, seqs):
    heads, total, _ = query.shape
    rows, width = total // seqs, HEADS * HEAD_DIM

    def body(q_ref, k_ref, sums_ref, g_ref, c_ref, s_ref, out_ref, row_ref, head_ref):
        cos, sin = c_ref[...], s_ref[...]
        everyone = sums_ref[0]
        for other in range(1, sums_ref.shape[0]):
            everyone = everyone + sums_ref[other]
        scale = lax.rsqrt(everyone / width + 1e-06)
        for which, x_ref in enumerate((q_ref, k_ref)):
            row_ref[...] = jnp.broadcast_to(scale[which : which + 1, :], (HEAD_DIM, total)).T
            for h in range(heads):
                head_ref[h] = x_ref[h] * row_ref[...] * g_ref[which, h : h + 1, :]
                for j in range(seqs):
                    part = head_ref[h, pl.ds(j, rows, stride=seqs), :]
                    turned = part * cos + pltpu.roll(part, HALF, 1) * sin
                    out_ref[j * heads + h, which] = turned.astype(jnp.bfloat16)

    return pl.pallas_call(
        body,
        out_shape=jax.ShapeDtypeStruct((slots, 2, rows, HEAD_DIM), jnp.bfloat16),
        scratch_shapes=[
            pltpu.VMEM((total, HEAD_DIM), jnp.float32),
            pltpu.VMEM((heads, total, HEAD_DIM), jnp.float32),
        ],
        compiler_params=pltpu.CompilerParams(vmem_limit_bytes=16 << 20),
        name="pack",
    )(query, key, sums, gains, cosine, sine)


def attend(query_key, value):
    blocks, rows, _ = value.shape
    per = BLOCK // rows
    steps = blocks // per
    power = HEAD_DIM ** (-0.5) * LOG2E

    def body(in_ref, v_ref, out_ref, s_ref, p_ref):
        row = lax.broadcasted_iota(jnp.int32, (BLOCK, BLOCK), 0)
        col = lax.broadcasted_iota(jnp.int32, (BLOCK, BLOCK), 1)

        def score(i, c, top):
            q = in_ref[per * i : per * (i + 1), 0].reshape(BLOCK, HEAD_DIM)
            k = in_ref[per * c : per * (c + 1), 1].reshape(BLOCK, HEAD_DIM)
            s = lax.dot_general(q, k, (((1,), (1,)), ((), ())), preferred_element_type=jnp.float32)
            if c == i:
                s = jnp.where(col <= row, s, -1e30)
            s_ref[i % 2, :, c * BLOCK : (c + 1) * BLOCK] = s
            best = jnp.maximum(s[:, :HEAD_DIM], s[:, HEAD_DIM:])
            return best if top is None else jnp.maximum(top, best)

        def weigh(i, c, top, total):
            e = jnp.exp2((s_ref[i % 2, :, c * BLOCK : (c + 1) * BLOCK] - top) * power)
            p_ref[i % 2, :, c * BLOCK : (c + 1) * BLOCK] = e.astype(jnp.bfloat16)
            here = e[:, :HEAD_DIM] + e[:, HEAD_DIM:]
            return here if total is None else total + here

        top = score(0, 0, None)
        for i in range(steps):
            best = jnp.max(top, axis=1, keepdims=True)
            top, total = None, None
            for c in range(i + 2):
                if i + 1 < steps:
                    top = score(i + 1, c, top)
                if c <= i:
                    total = weigh(i, c, best, total)
            v = v_ref[: per * (i + 1)].reshape(BLOCK * (i + 1), HEAD_DIM)
            acc = jnp.dot(p_ref[i % 2, :, : BLOCK * (i + 1)], v, preferred_element_type=jnp.float32)
            mixed = acc / jnp.sum(total, axis=1, keepdims=True)
            out_ref[per * i : per * (i + 1)] = mixed.astype(jnp.bfloat16).reshape(per, rows, HEAD_DIM)

    return pl.pallas_call(
        body,
        out_shape=jax.ShapeDtypeStruct((blocks, rows, HEAD_DIM), jnp.bfloat16),
        scratch_shapes=[
            pltpu.VMEM((2, BLOCK, blocks * rows), jnp.float32),
            pltpu.VMEM((2, BLOCK, blocks * rows), jnp.bfloat16),
        ],
        compiler_params=pltpu.CompilerParams(vmem_limit_bytes=16 << 20),
        cost_estimate=pl.CostEstimate(
            flops=64 * (blocks * rows) ** 2 * HEAD_DIM,
            transcendentals=(blocks * rows) ** 2 // 2,
            bytes_accessed=8 * blocks * rows * HEAD_DIM,
        ),
        name="attend",
    )(query_key, value)


def project_out(parts, weight, seqs):
    rows = parts.shape[1]
    local_width, depth = weight.shape
    heads = local_width // HEAD_DIM
    wide = 512

    def body(in_ref, w_ref, out_ref, head_ref, x_ref):
        for h in range(heads):
            for j in range(seqs):
                head_ref[h, pl.ds(j, rows, stride=seqs), :] = in_ref[j * heads + h].astype(jnp.float32)
            x_ref[:, h * HEAD_DIM : (h + 1) * HEAD_DIM] = head_ref[h].astype(jnp.bfloat16)

        def step(n, _):
            columns = pl.ds(pl.multiple_of(n * wide, wide), wide)
            got = jnp.dot(x_ref[...], w_ref[:, columns], preferred_element_type=jnp.float32)
            out_ref[:, columns] = got.astype(jnp.bfloat16)
            return 0

        lax.fori_loop(0, depth // wide, step, 0)

    vmem = pl.BlockSpec(memory_space=pltpu.VMEM)
    return pl.pallas_call(
        body,
        in_specs=[vmem, vmem],
        out_specs=vmem,
        out_shape=jax.ShapeDtypeStruct((rows * seqs, depth), jnp.bfloat16),
        scratch_shapes=[
            pltpu.VMEM((heads, rows * seqs, HEAD_DIM), jnp.float32),
            pltpu.VMEM((rows * seqs, local_width), jnp.bfloat16),
        ],
        compiler_params=pltpu.CompilerParams(vmem_limit_bytes=8 << 20),
        cost_estimate=pl.CostEstimate(
            flops=2 * rows * seqs * local_width * depth, transcendentals=0, bytes_accessed=2 * local_width * depth
        ),
        name="project_out",
    )(parts, weight)


def exchange(array, axis):
    return lax.all_to_all(array, axis, 0, 0, tiled=True)


def local(tokens, w_query, w_key, w_value, w_out, gain_query, gain_key):
    rows, seqs, depth = tokens.shape
    heads = w_query.shape[1] // HEAD_DIM
    slots, fold = lax.axis_size("seq"), lax.axis_size("tensor")
    first_token = (lax.axis_index("seq") * rows).astype(jnp.int32)[None]
    gains = jnp.stack([gain_query, gain_key]).reshape(2, heads, HEAD_DIM)

    flat, sent_v = project_value(tokens, w_value, slots)
    got_v = exchange(sent_v, "seq")
    query, key_raw, squares = project_query_key(flat, w_query, w_key)
    cosine, sine = turn_tables(first_token, rows)
    others = [
        lax.ppermute(squares, "tensor", [(i, (i + shift) % fold) for i in range(fold)])
        for shift in range(1, fold)
    ]
    sent_qk = pack(query, key_raw, jnp.stack([squares, *others]), gains, cosine, sine, slots, seqs)
    mixed = exchange(attend(exchange(sent_qk, "seq"), got_v), "seq")
    partial = project_out(mixed, w_out, seqs)
    pieces = exchange(partial.reshape(fold, -1, depth), "tensor")
    attended = jnp.sum(pieces.astype(jnp.float32), axis=0).astype(jnp.bfloat16)
    return attended.reshape(-1, seqs, depth)


def solution(mesh):
    return jax.shard_map(
        local,
        mesh=mesh,
        in_specs=(
            P("seq", "dp", None),
            P(None, "tensor"),
            P(None, "tensor"),
            P(None, "tensor"),
            P("tensor", None),
            P("tensor"),
            P("tensor"),
        ),
        out_specs=P(("seq", "tensor"), "dp", None),
        check_vma=False,
    )
```

```python
import jax
import jax.numpy as jnp
from jax import lax
from jax.experimental import pallas as pl
from jax.experimental.pallas import tpu as pltpu
from jax.sharding import PartitionSpec as P


HEADS = 40
HEAD_DIM = 128
HALF = HEAD_DIM // 2
LOG2E = 1.4426950408889634
BLOCK = 256
AHEAD = 4
ROWS_IN = 512


def row_of(column):
    return jnp.sum(column.T, axis=0, keepdims=True)


def in_hbm(array):
    return pltpu.with_memory_space_constraint(array, pltpu.HBM)


def stream(x_ref, weights, sums, buffer, arrived, before, beside):
    block = buffer.shape[1]
    blocks = weights[0].shape[0] // block

    def copy(which, n):
        at = (which * blocks + n) % (AHEAD + 1)
        return pltpu.make_async_copy(weights[which].at[pl.ds(n * block, block), :], buffer.at[at], arrived.at[at])

    for n in range(AHEAD):
        copy(0, n).start()
    before()
    for which in range(len(weights)):

        def step(n, _, which=which):
            @pl.when(n + AHEAD < blocks)
            def _():
                copy(which, n + AHEAD).start()

            if which + 1 < len(weights):

                @pl.when(n + AHEAD >= blocks)
                def _():
                    copy(which + 1, n + AHEAD - blocks).start()

            copy(which, n).wait()
            columns = pl.ds(pl.multiple_of(n * block, block), block)
            part = buffer[(which * blocks + n) % (AHEAD + 1)]
            sums[which][...] += jnp.dot(x_ref[:, columns], part, preferred_element_type=jnp.float32)
            beside(jnp.minimum(n + 1, blocks - 1))
            return 0

        sums[which][...] = jnp.zeros_like(sums[which])
        lax.fori_loop(0, blocks, step, 0)


def project_value(tokens, weight, slots):
    rows, seqs, depth = tokens.shape
    total, width = rows * seqs, weight.shape[1]
    heads = width // HEAD_DIM

    def body(in_ref, w_ref, x_ref, out_ref, sums, buffer, arrived, head_ref, token_ref, here):
        tokens_in = pltpu.make_async_copy(in_ref, token_ref, here)
        tokens_in.start()

        def rows_of(n):
            columns = pl.ds(pl.multiple_of(n * ROWS_IN, ROWS_IN), ROWS_IN)
            x_ref[:, columns] = token_ref[:, :, columns].reshape(total, ROWS_IN)

        def before():
            tokens_in.wait()
            rows_of(0)

        stream(x_ref, (w_ref,), (sums,), buffer, arrived, before, rows_of)
        for h in range(heads):
            head_ref[h] = sums[:, h * HEAD_DIM : (h + 1) * HEAD_DIM]
            for j in range(seqs):
                out_ref[j * heads + h] = head_ref[h, pl.ds(j, rows, stride=seqs), :].astype(jnp.bfloat16)

    vmem = pl.BlockSpec(memory_space=pltpu.VMEM)
    return pl.pallas_call(
        body,
        in_specs=[pl.BlockSpec(memory_space=pltpu.HBM)] * 2,
        out_specs=[vmem, vmem],
        out_shape=[
            jax.ShapeDtypeStruct((total, depth), jnp.bfloat16),
            jax.ShapeDtypeStruct((slots, rows, HEAD_DIM), jnp.bfloat16),
        ],
        scratch_shapes=[
            pltpu.VMEM((total, width), jnp.float32),
            pltpu.VMEM((AHEAD + 1, ROWS_IN, width), jnp.bfloat16),
            pltpu.SemaphoreType.DMA((AHEAD + 1,)),
            pltpu.VMEM((heads, total, HEAD_DIM), jnp.float32),
            pltpu.VMEM(tokens.shape, jnp.bfloat16),
            pltpu.SemaphoreType.DMA,
        ],
        compiler_params=pltpu.CompilerParams(vmem_limit_bytes=24 << 20),
        name="project_value",
    )(in_hbm(tokens), in_hbm(weight))


def turn_tables(first_token, rows):
    def body(at_ref, c_ref, s_ref):
        lane = lax.broadcasted_iota(jnp.int32, (rows, HEAD_DIM), 1)
        token = at_ref[0] + lax.broadcasted_iota(jnp.int32, (rows, HEAD_DIM), 0)
        pair = jnp.where(lane < HALF, lane, lane - HALF).astype(jnp.float32)
        angle = token.astype(jnp.float32) * jnp.exp(-jnp.log(500000.0) * pair * 2.0 / HEAD_DIM)
        c_ref[...] = jnp.cos(angle)
        s_ref[...] = jnp.where(lane < HALF, -jnp.sin(angle), jnp.sin(angle))

    return pl.pallas_call(
        body,
        in_specs=[pl.BlockSpec(memory_space=pltpu.SMEM)],
        out_shape=[jax.ShapeDtypeStruct((rows, HEAD_DIM), jnp.float32)] * 2,
        compiler_params=pltpu.CompilerParams(vmem_limit_bytes=4 << 20),
        name="turn_tables",
    )(first_token)


def project_query_key(flat, w_query, w_key):
    total, _ = flat.shape
    heads = w_query.shape[1] // HEAD_DIM

    def body(x_ref, wq_ref, wk_ref, q_ref, k_ref, sums_ref, sums, buffer, arrived):
        stream(x_ref, (wq_ref, wk_ref), (sums.at[0], sums.at[1]), buffer, arrived, lambda: None, lambda n: None)
        squares = []
        for which, out_ref in enumerate((q_ref, k_ref)):
            square = jnp.zeros((total, HEAD_DIM), jnp.float32)
            for h in range(heads):
                part = sums[which, :, h * HEAD_DIM : (h + 1) * HEAD_DIM]
                out_ref[h] = part
                square = square + part * part
            squares.append(row_of(square))
        sums_ref[...] = jnp.concatenate(squares * 4, axis=0)

    vmem, hbm = pl.BlockSpec(memory_space=pltpu.VMEM), pl.BlockSpec(memory_space=pltpu.HBM)
    return pl.pallas_call(
        body,
        in_specs=[vmem, hbm, hbm],
        out_specs=[vmem] * 3,
        out_shape=[
            jax.ShapeDtypeStruct((heads, total, HEAD_DIM), jnp.float32),
            jax.ShapeDtypeStruct((heads, total, HEAD_DIM), jnp.float32),
            jax.ShapeDtypeStruct((8, total), jnp.float32),
        ],
        scratch_shapes=[
            pltpu.VMEM((2, total, heads * HEAD_DIM), jnp.float32),
            pltpu.VMEM((AHEAD + 1, ROWS_IN, heads * HEAD_DIM), jnp.bfloat16),
            pltpu.SemaphoreType.DMA((AHEAD + 1,)),
        ],
        compiler_params=pltpu.CompilerParams(vmem_limit_bytes=24 << 20),
        name="project_query_key",
    )(flat, in_hbm(w_query), in_hbm(w_key))


def pack(query, key, sums, gains, cosine, sine, slots, seqs):
    heads, total, _ = query.shape
    rows, width = total // seqs, HEADS * HEAD_DIM

    def body(q_ref, k_ref, sums_ref, g_ref, c_ref, s_ref, out_ref, row_ref, head_ref):
        cos, sin = c_ref[...], s_ref[...]
        everyone = sums_ref[0]
        for other in range(1, sums_ref.shape[0]):
            everyone = everyone + sums_ref[other]
        scale = lax.rsqrt(everyone / width + 1e-06)
        for which, x_ref in enumerate((q_ref, k_ref)):
            row_ref[...] = jnp.broadcast_to(scale[which : which + 1, :], (HEAD_DIM, total)).T
            for h in range(heads):
                head_ref[h] = x_ref[h] * row_ref[...] * g_ref[which, h : h + 1, :]
                for j in range(seqs):
                    part = head_ref[h, pl.ds(j, rows, stride=seqs), :]
                    turned = part * cos + pltpu.roll(part, HALF, 1) * sin
                    out_ref[j * heads + h, which] = turned.astype(jnp.bfloat16)

    return pl.pallas_call(
        body,
        out_shape=jax.ShapeDtypeStruct((slots, 2, rows, HEAD_DIM), jnp.bfloat16),
        scratch_shapes=[
            pltpu.VMEM((total, HEAD_DIM), jnp.float32),
            pltpu.VMEM((heads, total, HEAD_DIM), jnp.float32),
        ],
        compiler_params=pltpu.CompilerParams(vmem_limit_bytes=16 << 20),
        name="pack",
    )(query, key, sums, gains, cosine, sine)


def attend(query_key, value):
    blocks, rows, _ = value.shape
    per = BLOCK // rows
    steps = blocks // per
    power = HEAD_DIM ** (-0.5) * LOG2E

    def body(in_ref, v_ref, out_ref, s_ref, p_ref):
        row = lax.broadcasted_iota(jnp.int32, (BLOCK, BLOCK), 0)
        col = lax.broadcasted_iota(jnp.int32, (BLOCK, BLOCK), 1)

        def score(i, c, top):
            q = in_ref[per * i : per * (i + 1), 0].reshape(BLOCK, HEAD_DIM)
            k = in_ref[per * c : per * (c + 1), 1].reshape(BLOCK, HEAD_DIM)
            s = lax.dot_general(q, k, (((1,), (1,)), ((), ())), preferred_element_type=jnp.float32)
            if c == i:
                s = jnp.where(col <= row, s, -1e30)
            s_ref[i % 2, :, c * BLOCK : (c + 1) * BLOCK] = s
            best = jnp.maximum(s[:, :HEAD_DIM], s[:, HEAD_DIM:])
            return best if top is None else jnp.maximum(top, best)

        def weigh(i, c, top, total):
            e = jnp.exp2((s_ref[i % 2, :, c * BLOCK : (c + 1) * BLOCK] - top) * power)
            p_ref[i % 2, :, c * BLOCK : (c + 1) * BLOCK] = e.astype(jnp.bfloat16)
            here = e[:, :HEAD_DIM] + e[:, HEAD_DIM:]
            return here if total is None else total + here

        top = score(0, 0, None)
        for i in range(steps):
            best = jnp.max(top, axis=1, keepdims=True)
            top, total = None, None
            for c in range(i + 2):
                if i + 1 < steps:
                    top = score(i + 1, c, top)
                if c <= i:
                    total = weigh(i, c, best, total)
            v = v_ref[: per * (i + 1)].reshape(BLOCK * (i + 1), HEAD_DIM)
            acc = jnp.dot(p_ref[i % 2, :, : BLOCK * (i + 1)], v, preferred_element_type=jnp.float32)
            mixed = acc / jnp.sum(total, axis=1, keepdims=True)
            out_ref[per * i : per * (i + 1)] = mixed.astype(jnp.bfloat16).reshape(per, rows, HEAD_DIM)

    return pl.pallas_call(
        body,
        out_shape=jax.ShapeDtypeStruct((blocks, rows, HEAD_DIM), jnp.bfloat16),
        scratch_shapes=[
            pltpu.VMEM((2, BLOCK, blocks * rows), jnp.float32),
            pltpu.VMEM((2, BLOCK, blocks * rows), jnp.bfloat16),
        ],
        compiler_params=pltpu.CompilerParams(vmem_limit_bytes=16 << 20),
        cost_estimate=pl.CostEstimate(
            flops=64 * (blocks * rows) ** 2 * HEAD_DIM,
            transcendentals=(blocks * rows) ** 2 // 2,
            bytes_accessed=8 * blocks * rows * HEAD_DIM,
        ),
        name="attend",
    )(query_key, value)


def project_out(parts, weight, seqs):
    rows = parts.shape[1]
    local_width, depth = weight.shape
    heads = local_width // HEAD_DIM
    wide = 512

    def body(in_ref, w_ref, out_ref, head_ref, x_ref):
        for h in range(heads):
            for j in range(seqs):
                head_ref[h, pl.ds(j, rows, stride=seqs), :] = in_ref[j * heads + h].astype(jnp.float32)
            x_ref[:, h * HEAD_DIM : (h + 1) * HEAD_DIM] = head_ref[h].astype(jnp.bfloat16)

        def step(n, _):
            columns = pl.ds(pl.multiple_of(n * wide, wide), wide)
            got = jnp.dot(x_ref[...], w_ref[:, columns], preferred_element_type=jnp.float32)
            out_ref[:, columns] = got.astype(jnp.bfloat16)
            return 0

        lax.fori_loop(0, depth // wide, step, 0)

    vmem = pl.BlockSpec(memory_space=pltpu.VMEM)
    return pl.pallas_call(
        body,
        in_specs=[vmem, vmem],
        out_specs=vmem,
        out_shape=jax.ShapeDtypeStruct((rows * seqs, depth), jnp.bfloat16),
        scratch_shapes=[
            pltpu.VMEM((heads, rows * seqs, HEAD_DIM), jnp.float32),
            pltpu.VMEM((rows * seqs, local_width), jnp.bfloat16),
        ],
        compiler_params=pltpu.CompilerParams(vmem_limit_bytes=8 << 20),
        cost_estimate=pl.CostEstimate(
            flops=2 * rows * seqs * local_width * depth, transcendentals=0, bytes_accessed=2 * local_width * depth
        ),
        name="project_out",
    )(parts, weight)


def add_up(pieces, seqs):
    count, total, depth = pieces.shape

    def body(in_ref, out_ref):
        whole = in_ref[0].astype(jnp.float32)
        for other in range(1, count):
            whole = whole + in_ref[other].astype(jnp.float32)
        out_ref[...] = whole.astype(jnp.bfloat16).reshape(total // seqs, seqs, depth)

    return pl.pallas_call(
        body,
        out_shape=jax.ShapeDtypeStruct((total // seqs, seqs, depth), jnp.bfloat16),
        compiler_params=pltpu.CompilerParams(vmem_limit_bytes=8 << 20),
        name="add_up",
    )(pieces)


def exchange(array, axis):
    return lax.all_to_all(array, axis, 0, 0, tiled=True)


def local(tokens, w_query, w_key, w_value, w_out, gain_query, gain_key):
    rows, seqs, depth = tokens.shape
    heads = w_query.shape[1] // HEAD_DIM
    slots, fold = lax.axis_size("seq"), lax.axis_size("tensor")
    first_token = (lax.axis_index("seq") * rows).astype(jnp.int32)[None]
    gains = jnp.stack([gain_query, gain_key]).reshape(2, heads, HEAD_DIM)

    flat, sent_v = project_value(tokens, w_value, slots)
    got_v = exchange(sent_v, "seq")
    query, key_raw, squares = project_query_key(flat, w_query, w_key)
    cosine, sine = turn_tables(first_token, rows)
    others = [
        lax.ppermute(squares, "tensor", [(i, (i + shift) % fold) for i in range(fold)])
        for shift in range(1, fold)
    ]
    sent_qk = pack(query, key_raw, jnp.stack([squares, *others]), gains, cosine, sine, slots, seqs)
    mixed = exchange(attend(exchange(sent_qk, "seq"), got_v), "seq")
    partial = project_out(mixed, w_out, seqs)
    pieces = exchange(partial.reshape(fold, -1, depth), "tensor")
    return add_up(pieces, seqs)


def solution(mesh):
    return jax.shard_map(
        local,
        mesh=mesh,
        in_specs=(
            P("seq", "dp", None),
            P(None, "tensor"),
            P(None, "tensor"),
            P(None, "tensor"),
            P("tensor", None),
            P("tensor"),
            P("tensor"),
        ),
        out_specs=P(("seq", "tensor"), "dp", None),
        check_vma=False,
    )
```
